32 devices in a mesh: reg: 4 (over y, core), prod: 8 (over z, x).
Axes of the slice: x: 2, y: 2, z: 4, core: 2. Of those that a mesh axis runs over, the one named last changes fastest.
Arguments:
- bottom_series_predictions: float32 [128, 256, 128], P('reg', 'prod'), may hold values from -6 to 6
- group_item_predictions: float32 [32, 256, 128], P('reg', 'prod'), may hold values from -18 to 18
- area_class_predictions: float32 [128, 32, 128], P('reg', 'prod'), may hold values from -18 to 18
- group_class_predictions: float32 [32, 32, 128], P('reg'), may hold values from -48 to 48
- bottom_series_precision: float32 [128, 256], P('reg', 'prod'), may hold values from 0.5 to 5
- group_item_precision: float32 [32, 256], P('reg', 'prod'), may hold values from 0.02 to 0.5
- area_class_precision: float32 [128, 32], P('reg', 'prod'), may hold values from 0.02 to 0.5
- group_class_precision: float32 [32, 32], P('reg'), may hold values from 0.002 to 0.05
- group_area_partition: int32 [32, 128], replicated, may hold values from -1 to 127, as said below
- class_item_partition: int32 [32, 128], replicated, may hold values from -1 to 255, as said below
Outputs:
- solution_field: float32 [128, 256, 128], P('reg', 'prod')
- residual: float32 [128, 256, 128], P('reg', 'prod')
The draws below stay inside these ranges and needn't reach their ends.
Inputs may be any that keep to these rules, and one draw needn't show every extreme that they name: `group_area_partition`: every region stands in exactly one row; each row holds its parent's regions in its first slots and -1 in the rest; a parent has 1 to 97 regions, and some parent has exactly 97. `class_item_partition`: every product stands in exactly one row; each row holds its category's products in its first slots and -1 in the rest; a category has 1 to 128 products, and some category has exactly 128.
All inputs are finite; a program needn't handle non-finite values.
Results may differ from the reference program's by a relative error of at most 0.00011.
Values sent between devices are 32-bit elements; how exact they have to be, the bound alone decides.
A program may use at most 64 MiB of HBM per device.

```python
import math
import jax
import jax.numpy as jnp
from jax import lax

HORIZON_PERIODS = 128
AREA_GROUPS = 32
GOODS_CLASSES = 32
CHILD_SLOTS = 128
ITERATIONS = 2
AREA_NUMBER = 128
ITEM_NUMBER = 256
REGION_MOST = 97
PRODUCT_MOST = 128


def children_table(key, items, groups, slots, most):
    order = jax.random.permutation(jax.random.fold_in(key, 11), items).astype(jnp.int32)
    others = groups - 1
    remain = items - most
    base = remain // others
    extra = remain % others
    rest = base + (jnp.arange(others, dtype=jnp.int32) < extra).astype(jnp.int32)
    pairs = others // 2
    halves = jax.random.randint(jax.random.fold_in(key, 12), (pairs,), -(base // 2), base // 2 + 1, dtype=jnp.int32)
    delta = jnp.stack([halves, -halves], axis=1).reshape(2 * pairs)
    delta = jnp.concatenate([delta, jnp.zeros((others - 2 * pairs,), jnp.int32)])
    rest = rest + delta
    chosen = jax.random.randint(jax.random.fold_in(key, 13), (), 0, groups, dtype=jnp.int32)
    group_ids = jnp.arange(groups, dtype=jnp.int32)
    source = jnp.clip(group_ids - (group_ids > chosen).astype(jnp.int32), 0, others - 1)
    counts = jnp.where(group_ids == chosen, most, rest[source]).astype(jnp.int32)
    starts = jnp.cumsum(counts) - counts
    slot = jnp.arange(slots, dtype=jnp.int32)
    where_at = starts[:, None] + slot[None, :]
    valid = slot[None, :] < counts[:, None]
    picked = order[jnp.clip(where_at, 0, items - 1)]
    return jnp.where(valid, picked, -1).astype(jnp.int32)


def draw_group_area_partition(key, part):
    return children_table(jax.random.fold_in(key, 101), AREA_NUMBER, AREA_GROUPS, CHILD_SLOTS, REGION_MOST)


def draw_class_item_partition(key, part):
    return children_table(jax.random.fold_in(key, 202), ITEM_NUMBER, GOODS_CLASSES, CHILD_SLOTS, PRODUCT_MOST)


def block_levels(key, shape, split, smallest, top_value):
    def one(position, blocks):
        steps = jax.random.uniform(jax.random.fold_in(jax.random.fold_in(key, 6), position), (blocks,), jnp.float32, smallest / len(split), top_value / len(split))
        return jnp.repeat(jnp.exp(steps), shape[position] // blocks).reshape((-1,) + (1,) * (len(shape) - position - 1))

    factor_of = one(*split[0])
    for cut in split[1:]:
        factor_of = factor_of * one(*cut)
    return factor_of


def centred(stream_key, extent, scale, most, shards=(), kind=jnp.bfloat16):
    result = scale * jax.random.normal(stream_key, extent, jnp.float32)
    if shards:
        result = result * block_levels(stream_key, extent, shards, -0.22, 0.18)
    return jnp.clip(result, -most, most).astype(kind)


def setup_inputs(seed: int = 0) -> dict:
    arg_keys = jax.random.split(jax.random.key(seed), 11)
    bottom_series_predictions = centred(arg_keys[0], (AREA_NUMBER, ITEM_NUMBER, HORIZON_PERIODS), 1.0, 6.0, ((0, 4), (1, 8)), jnp.float32)
    group_item_predictions = centred(arg_keys[1], (AREA_GROUPS, ITEM_NUMBER, HORIZON_PERIODS), 3.0, 18.0, ((0, 4), (1, 8)), jnp.float32)
    area_class_predictions = centred(arg_keys[2], (AREA_NUMBER, GOODS_CLASSES, HORIZON_PERIODS), 3.0, 18.0, ((0, 4), (1, 8)), jnp.float32)
    group_class_predictions = centred(arg_keys[3], (AREA_GROUPS, GOODS_CLASSES, HORIZON_PERIODS), 8.0, 48.0, ((0, 4),), jnp.float32)
    bottom_series_precision = jnp.clip(jnp.exp(math.log(5.0) - 2.3025851 * jax.random.uniform(arg_keys[4], (AREA_NUMBER, ITEM_NUMBER), jnp.float32) ** block_levels(arg_keys[4], (AREA_NUMBER, ITEM_NUMBER), ((0, 4), (1, 8)), -0.2, 0.2)), 0.5, 5.0)
    group_item_precision = jnp.clip(jnp.exp(math.log(0.5) - 3.218876 * jax.random.uniform(arg_keys[5], (AREA_GROUPS, ITEM_NUMBER), jnp.float32) ** block_levels(arg_keys[5], (AREA_GROUPS, ITEM_NUMBER), ((0, 4), (1, 8)), -0.2, 0.2)), 0.02, 0.5)
    area_class_precision = jnp.clip(jnp.exp(math.log(0.5) - 3.218876 * jax.random.uniform(arg_keys[6], (AREA_NUMBER, GOODS_CLASSES), jnp.float32) ** block_levels(arg_keys[6], (AREA_NUMBER, GOODS_CLASSES), ((0, 4), (1, 8)), -0.2, 0.2)), 0.02, 0.5)
    group_class_precision = jnp.clip(jnp.exp(math.log(0.05) - 3.218876 * jax.random.uniform(arg_keys[7], (AREA_GROUPS, GOODS_CLASSES), jnp.float32) ** block_levels(arg_keys[7], (AREA_GROUPS, GOODS_CLASSES), ((0, 4),), -0.2, 0.2)), 0.002, 0.05)
    group_area_partition = draw_group_area_partition(jax.random.fold_in(arg_keys[10], 71), 0)
    class_item_partition = draw_class_item_partition(jax.random.fold_in(arg_keys[10], 71), 0)
    return {"bottom_series_predictions": bottom_series_predictions, "group_item_predictions": group_item_predictions, "area_class_predictions": area_class_predictions, "group_class_predictions": group_class_predictions, "bottom_series_precision": bottom_series_precision, "group_item_precision": group_item_precision, "area_class_precision": area_class_precision, "group_class_precision": group_class_precision, "group_area_partition": group_area_partition, "class_item_partition": class_item_partition}


def member_map(table, count):
    items = jnp.arange(count, dtype=jnp.int32)
    return jnp.any(table[:, :, None] == items[None, None, :], axis=1).astype(jnp.float32)


def aggregate_upward(area_index_table, item_index_table, upper, lower, corner):
    high = lax.Precision.HIGHEST
    widened = upper + jnp.einsum('pch,cq->pqh', corner, item_index_table, precision=high)
    first = jnp.einsum('pr,pqh->rqh', area_index_table, widened, precision=high)
    second = jnp.einsum('rch,cq->rqh', lower, item_index_table, precision=high)
    return first + second


def reference(bottom_series_predictions, group_item_predictions, area_class_predictions, group_class_predictions, bottom_series_precision, group_item_precision, area_class_precision, group_class_precision, group_area_partition, class_item_partition):
    high = lax.Precision.HIGHEST
    area_index_table = member_map(group_area_partition, AREA_NUMBER)
    item_index_table = member_map(class_item_partition, ITEM_NUMBER)

    def operate(field):
        row_total = jnp.einsum('pr,rqh->pqh', area_index_table, field, precision=high)
        col_total = jnp.einsum('cq,rqh->rch', item_index_table, field, precision=high)
        corner_total = jnp.einsum('pqh,cq->pch', row_total, item_index_table, precision=high)
        disaggregate_onto = aggregate_upward(area_index_table, item_index_table, group_item_precision[:, :, None] * row_total, area_class_precision[:, :, None] * col_total, group_class_precision[:, :, None] * corner_total)
        return bottom_series_precision[:, :, None] * field + disaggregate_onto

    system_source_term = bottom_series_precision[:, :, None] * bottom_series_predictions + aggregate_upward(area_index_table, item_index_table, group_item_precision[:, :, None] * group_item_predictions, area_class_precision[:, :, None] * area_class_predictions, group_class_precision[:, :, None] * group_class_predictions)
    solution_field = jnp.zeros_like(system_source_term)
    residual, direction = system_source_term, system_source_term
    norm_now = jnp.sum(residual * residual)
    for step in range(ITERATIONS):
        image = operate(direction)
        alpha = norm_now / jnp.sum(direction * image)
        solution_field = solution_field + alpha * direction
        residual = residual - alpha * image
        norm_next = jnp.sum(residual * residual)
        direction = residual + (norm_next / norm_now) * direction
        norm_now = norm_next
    return solution_field, residual
```

```python
import functools

import jax
import jax.numpy as jnp
from jax import lax
from jax.experimental import pallas as pl
from jax.experimental.pallas import tpu as pltpu
from jax.sharding import PartitionSpec as P

MESH = pl.DeviceIdType.MESH
ITERATIONS = 2
LANES = 128


def halves(x):
    hi = x.astype(jnp.bfloat16)
    lo = (x - hi.astype(jnp.float32)).astype(jnp.bfloat16)
    return jnp.concatenate([hi, lo], axis=0)


def apply_map(map2, x):
    return jnp.dot(map2, halves(x), preferred_element_type=jnp.float32)


def kernel(
    nr, np_, shared, per_tile,
    par_ref, kidx_ref, mask_ref,
    b_ref, dt_ref, u_ref, z_ref, v_ref, wt_ref, at_ref, rs_ref, p2_ref, pt2_ref, e2_ref,
    x_ref, res_ref,
    wt_buf, at_buf, uz_buf, g0_buf, uz_send,
    db, wcol, wgi, wgc, r0_buf, img0, img1,
    col_send, rs_buf, own, vbuf, gbuf, row_send, row_buf, rows_w, cor_send, cor_buf, zed,
    sc_send, sc_buf, sd_send, sd_buf,
    s_w, r_w, s_uz, r_uz, s_a, r_a, s_v, r_v,
    s_rs, r_rs, s_ag, r_ag, s_row, r_row, s_cor, r_cor, s_sc, r_sc, s_sd, r_sd,
):
    regions, items, horizon = b_ref.shape
    classes = p2_ref.shape[0]
    slab = regions // np_
    gs = u_ref.shape[0]
    mr = lax.axis_index("reg")
    mp = lax.axis_index("prod")

    def to(axis, me, n, s):
        return {axis: lax.rem(me + s, n)}

    def reg_copy(src, dst, ss, rr, s):
        return pltpu.make_async_remote_copy(
            src_ref=src, dst_ref=dst, send_sem=ss, recv_sem=rr,
            device_id=to("reg", mr, nr, s), device_id_type=MESH)

    def prod_copy(src, dst, ss, rr, s):
        return pltpu.make_async_remote_copy(
            src_ref=src, dst_ref=dst, send_sem=ss, recv_sem=rr,
            device_id=to("prod", mp, np_, s), device_id_type=MESH)

    barrier = pltpu.get_barrier_semaphore()
    for s in range(1, nr):
        pl.semaphore_signal(barrier, inc=1, device_id=to("reg", mr, nr, s), device_id_type=MESH)

    def greet(s, c):
        pl.semaphore_signal(barrier, inc=1, device_id=to("prod", mp, np_, s), device_id_type=MESH)
        return c

    lax.fori_loop(1, np_, greet, 0)
    for g in range(gs):
        uz_send[g] = u_ref[g] + apply_map(pt2_ref[...], z_ref[g])
    pl.semaphore_wait(barrier, nr - 1 + np_ - 1)

    def each_prod(f):
        lax.fori_loop(1, np_, lambda s, c: (f(s), c)[1], 0)

    def w_copy(s):
        return reg_copy(wt_ref, wt_buf.at[s], s_w.at[s], r_w.at[s], s)

    def uz_copy(s):
        return reg_copy(uz_send, uz_buf.at[pl.ds(mr * gs, gs)], s_uz.at[s], r_uz.at[s], s)

    def a_copy(s):
        return prod_copy(at_ref, at_buf.at[mp], s_a.at[s], r_a.at[s], s)

    def v_copy(s):
        return prod_copy(v_ref, g0_buf.at[mp], s_v.at[s], r_v.at[s], s)

    for s in range(1, nr):
        w_copy(s).start()
    each_prod(lambda s: v_copy(s).start())
    for s in range(1, nr):
        uz_copy(s).start()
    each_prod(lambda s: a_copy(s).start())
    g0_buf[mp] = v_ref[...]
    at_buf[mp] = at_ref[...]
    for g in range(gs):
        uz_buf[mr * gs + g] = uz_send[g]
    base = dt_ref[...]
    for r in range(regions):
        r0_buf[r] = jnp.broadcast_to(base[:, r : r + 1], (items, horizon)) * b_ref[r]
    total = wt_ref[...]
    for s in range(1, nr):
        w_copy(s).wait_recv()
        total = total + wt_buf[s]
    weights = jnp.dot(total, rs_ref[...], precision=lax.Precision.HIGHEST, preferred_element_type=jnp.float32)
    diag = base + weights[:items]
    for r in range(regions):
        db[r] = jnp.broadcast_to(diag[:, r : r + 1], (items, horizon))
    for k in range(shared):
        wgi[k] = jnp.broadcast_to(weights[:items, regions + k : regions + k + 1], (items, horizon))
        wgc[k] = jnp.broadcast_to(weights[items:, regions + k : regions + k + 1], (classes, horizon))

    each_prod(lambda s: a_copy(s).wait_recv())
    tiles = []
    for first in range(0, np_, per_tile):
        tile = at_buf[first]
        for j in range(first + 1, first + per_tile):
            tile = tile + at_buf[j]
        tiles.append(tile)
    wac = jnp.concatenate(tiles, axis=0) + weights[items:]
    lane = lax.broadcasted_iota(jnp.int32, (classes, LANES), 1)
    for i in range(slab):
        column = jnp.sum(jnp.where(lane == mp * slab + i, wac, 0.0), axis=1, keepdims=True)
        wcol[i] = jnp.broadcast_to(column, (classes, horizon))

    for s in range(1, nr):
        uz_copy(s).wait_recv()
    each_prod(lambda s: v_copy(s).wait_recv())

    def first_field(a, c):
        flat = jnp.concatenate([g0_buf[j, a] for j in range(np_)], axis=0)
        lifted = apply_map(e2_ref[...], flat)
        for t in range(per_tile):
            r = a * per_tile + t
            r0_buf[r] = r0_buf[r] + uz_buf[par_ref[r]] + lifted[t * items : (t + 1) * items]
        return c

    lax.fori_loop(0, regions // per_tile, first_field, 0)

    row_id = lax.broadcasted_iota(jnp.int32, (8, horizon), 0)
    norm_was = alpha_was = None
    for op in range(ITERATIONS):
        field = r0_buf if op == 0 else res_ref
        image = img0 if op == 0 else img1

        def row_copy(s, op=op):
            return reg_copy(row_send.at[op], row_buf.at[op, s], s_row.at[op, s], r_row.at[op, s], s)

        def rs_copy(s, op=op):
            return prod_copy(col_send.at[op, s], rs_buf.at[op, s], s_rs.at[op, s], r_rs.at[op, s], s)

        def cor_copy(s, op=op):
            return prod_copy(cor_send.at[op], cor_buf.at[op, s], s_cor.at[op, s], r_cor.at[op, s], s)

        def ag_copy(s, op=op):
            return prod_copy(vbuf.at[op], gbuf.at[op, pl.ds(mp * slab, slab)], s_ag.at[op, s], r_ag.at[op, s], s)

        def sc_copy(s, op=op):
            return reg_copy(sc_send.at[op], sc_buf.at[op, s], s_sc.at[op, s], r_sc.at[op, s], s)

        def sd_copy(s, op=op):
            return prod_copy(sd_send.at[op], sd_buf.at[op, s], s_sd.at[op, s], r_sd.at[op, s], s)

        def one_row(k, c, op=op, field=field):
            def add(r, acc):
                return acc + jnp.where(kidx_ref[r] == k, mask_ref[r], 0.0) * field[r]

            row_send[op, k] = lax.fori_loop(0, regions, add, jnp.zeros((items, horizon), jnp.float32))
            return c

        lax.fori_loop(0, shared, one_row, 0)
        for s in range(1, nr):
            row_copy(s).start()

        def columns(s, op=op, field=field):
            first = lax.rem(mp + s, np_) * slab
            wide = jnp.concatenate([field[first + i] for i in range(slab)], axis=1)
            out = apply_map(p2_ref[...], wide)
            return [out[:, i * horizon : (i + 1) * horizon] for i in range(slab)]

        def send_columns(s, op=op):
            for i, one in enumerate(columns(s)):
                col_send[op, s, i] = one
            rs_copy(s).start()

        each_prod(send_columns)
        for i, one in enumerate(columns(0)):
            own[i] = one

        for s in range(1, nr):
            row_copy(s).wait_recv()

        def one_corner(k, acc, op=op):
            rows = row_send[op, k]
            for s in range(1, nr):
                rows = rows + row_buf[op, s, k]
            weighted = wgi[k] * rows
            rows_w[k] = weighted
            cor_send[op, k] = apply_map(p2_ref[...], rows)
            return acc + weighted * rows

        row_part = lax.fori_loop(0, shared, one_corner, jnp.zeros((items, horizon), jnp.float32))
        each_prod(lambda s: cor_copy(s).start())

        def diagonal(r, acc, field=field, image=image):
            v = field[r]
            w = db[r] * v
            image[r] = w
            return acc[0] + v * v, acc[1] + w * v

        zero = jnp.zeros((items, horizon), jnp.float32)
        norm_part, along_part = lax.fori_loop(0, regions, diagonal, (zero, zero))
        along_part = along_part + row_part * (1.0 / nr)

        each_prod(lambda s: cor_copy(s).wait_recv())

        def one_zed(k, acc, op=op):
            corner = lax.fori_loop(1, np_, lambda s, c: c + cor_buf[op, s, k], cor_send[op, k])
            weighted = wgc[k] * corner
            zed[k] = weighted
            return acc + weighted * corner

        czero = jnp.zeros((classes, horizon), jnp.float32)
        cor_part = lax.fori_loop(0, shared, one_zed, czero) * (1.0 / (nr * np_))

        each_prod(lambda s: rs_copy(s).wait_recv())
        for i in range(slab):
            r = mp * slab + i
            cols = lax.fori_loop(1, np_, lambda s, c, i=i, op=op: c + rs_buf[op, s, i], own[i])
            weighted = wcol[i] * cols
            cor_part = cor_part + weighted * cols
            value = weighted + mask_ref[r] * zed[kidx_ref[r]]
            vbuf[op, i] = value
            gbuf[op, r] = value
        each_prod(lambda s: ag_copy(s).start())

        def fold(x):
            return jnp.sum(x, axis=0, keepdims=True)

        along_row = fold(along_part) + fold(cor_part)
        sc_send[op] = jnp.where(row_id == 0, fold(norm_part), jnp.where(row_id == 1, along_row, 0.0))
        for s in range(1, nr):
            sc_copy(s).start()
        tally = sc_send[op]
        for s in range(1, nr):
            sc_copy(s).wait_recv()
            tally = tally + sc_buf[op, s]
        sd_send[op] = tally
        each_prod(lambda s: sd_copy(s).start())

        def lift(first, op=op, image=image):
            wide = jnp.concatenate([gbuf[op, first + i] for i in range(slab)], axis=1)
            out = apply_map(pt2_ref[...], wide)
            for i in range(slab):
                r = first + i
                image[r] = (image[r] + mask_ref[r] * rows_w[kidx_ref[r]]) + out[:, i * horizon : (i + 1) * horizon]

        lift(mp * slab)

        def take(s, op=op):
            ag_copy(s).wait_recv()
            lift(lax.rem(mp - s + np_, np_) * slab)

        each_prod(take)
        each_prod(lambda s: sd_copy(s).wait_recv())
        tally = lax.fori_loop(1, np_, lambda s, c, op=op: c + sd_buf[op, s], sd_send[op])
        norm = jnp.sum(tally[0:1], axis=1, keepdims=True)
        along = jnp.sum(tally[1:2], axis=1, keepdims=True)
        if op == 0:
            alpha = norm / along

            def update(r, c, alpha=alpha):
                res_ref[r] = r0_buf[r] - alpha * img0[r]
                return c

            lax.fori_loop(0, regions, update, 0)
            norm_was, alpha_was = norm, alpha
        else:
            ratio = norm / norm_was
            alpha = norm / (along - ratio * norm / alpha_was)

            def finish(r, c, alpha=alpha, ratio=ratio):
                start, residual = r0_buf[r], res_ref[r]
                x_ref[r] = alpha_was * start + alpha * (residual + ratio * start)
                res_ref[r] = residual - alpha * (img1[r] + ratio * img0[r])
                return c

            lax.fori_loop(0, regions, finish, 0)

        for s in range(1, nr):
            row_copy(s).wait_send()
            sc_copy(s).wait_send()
        each_prod(lambda s: rs_copy(s).wait_send())
        each_prod(lambda s: cor_copy(s).wait_send())
        each_prod(lambda s: ag_copy(s).wait_send())
        each_prod(lambda s: sd_copy(s).wait_send())

    for s in range(1, nr):
        w_copy(s).wait_send()
        uz_copy(s).wait_send()
    each_prod(lambda s: a_copy(s).wait_send())
    each_prod(lambda s: v_copy(s).wait_send())


def on_device(nr, np_, bottom, gi_pred, ac_pred, gc_pred, bottom_w, gi_w, ac_w, gc_w, area_table, item_table):
    f32 = jnp.float32
    regions, items, horizon = bottom.shape
    groups, slots = area_table.shape
    classes = item_table.shape[0]
    gs, cs = gi_pred.shape[0], ac_pred.shape[1]
    slab = regions // np_
    per_tile = 8 // cs
    every = regions * nr
    most = min(slots, every - groups + 1)
    shared = 1 + min(groups - 1, every - most - (groups - 1))
    mr, mp = lax.axis_index("reg"), lax.axis_index("prod")

    def member(table, first, count):
        ids = first + jnp.arange(count, dtype=jnp.int32)
        return jnp.any(table[:, :, None] == ids[None, None, :], axis=1)

    area = member(area_table, mr * regions, regions)
    item = member(item_table, mp * items, items)
    sizes = jnp.sum((area_table >= 0).astype(jnp.int32), axis=1)
    ids = jnp.arange(groups, dtype=jnp.int32)
    ahead = (sizes[None, :] > sizes[:, None]) | ((sizes[None, :] == sizes[:, None]) & (ids[None, :] < ids[:, None]))
    rank = jnp.sum(ahead.astype(jnp.int32), axis=1)
    par = jnp.sum(jnp.where(area, ids[:, None], 0), axis=0)
    place = jnp.sum(jnp.where(area, rank[:, None], 0), axis=0)
    mask = (place < shared).astype(f32)
    kidx = jnp.minimum(place, shared - 1)
    single = (area & (rank[:, None] >= shared)).astype(f32)
    chosen = (rank[:, None] == jnp.arange(shared, dtype=jnp.int32)[None, :]).astype(f32)
    rs = jnp.concatenate([single, chosen], axis=1)
    rs = jnp.pad(rs, ((0, LANES - groups), (0, LANES - rs.shape[1])))

    itemf = item.astype(jnp.bfloat16)
    p2 = jnp.concatenate([itemf, itemf], axis=1)
    pt2 = jnp.concatenate([itemf.T, itemf.T], axis=1)
    by_owner = itemf.T.reshape(items, np_, 1, cs)
    eye = jnp.eye(per_tile, dtype=jnp.bfloat16)
    e = (eye[:, None, None, :, None] * by_owner[None]).reshape(per_tile * items, np_ * 8)
    e2 = jnp.concatenate([e, e], axis=1)

    weights = jnp.concatenate([gi_w.T, gc_w.T], axis=0)
    lanes = jnp.arange(LANES, dtype=jnp.int32)
    spread = (lanes[None, :] == mr * gs + jnp.arange(gs, dtype=jnp.int32)[:, None])
    wt = jnp.sum(jnp.where(spread[None], weights[:, :, None], 0.0), axis=1)
    spot = lax.rem(mp, per_tile) * cs + jnp.arange(cs, dtype=jnp.int32)
    rowsel = jnp.arange(8, dtype=jnp.int32)[:, None] == spot[None, :]
    at = jnp.sum(jnp.where(rowsel[:, :, None], ac_w.T[None], 0.0), axis=1)
    at = jnp.pad(at, ((0, 0), (0, LANES - regions)))
    dt = jnp.pad(bottom_w.T, ((0, 0), (0, LANES - regions)))
    u = gi_w[:, :, None] * gi_pred
    z = gc_w[:, :, None] * gc_pred
    v = (ac_w[:, :, None] * ac_pred).reshape(regions // per_tile, 8, horizon)

    field = (regions, items, horizon)
    two = ITERATIONS
    V = pltpu.VMEM
    dma = pltpu.SemaphoreType.DMA
    smem = pl.BlockSpec(memory_space=pltpu.SMEM)
    vmem = pl.BlockSpec(memory_space=pltpu.VMEM)
    return pl.pallas_call(
        functools.partial(kernel, nr, np_, shared, per_tile),
        out_shape=(jax.ShapeDtypeStruct(field, f32), jax.ShapeDtypeStruct(field, f32)),
        in_specs=[smem] * 3 + [vmem] * 11,
        out_specs=(vmem, vmem),
        scratch_shapes=[
            V((nr,) + wt.shape, f32),
            V((np_, 8, LANES), f32),
            V((groups, items, horizon), f32),
            V((np_, regions // per_tile, 8, horizon), f32),
            V((gs, items, horizon), f32),
            V(field, f32),
            V((slab, classes, horizon), f32),
            V((shared, items, horizon), f32),
            V((shared, classes, horizon), f32),
            V(field, f32),
            V(field, f32),
            V(field, f32),
            V((two, np_, slab, classes, horizon), f32),
            V((two, np_, slab, classes, horizon), f32),
            V((slab, classes, horizon), f32),
            V((two, slab, classes, horizon), f32),
            V((two, regions, classes, horizon), f32),
            V((two, shared, items, horizon), f32),
            V((two, nr, shared, items, horizon), f32),
            V((shared, items, horizon), f32),
            V((two, shared, classes, horizon), f32),
            V((two, np_, shared, classes, horizon), f32),
            V((shared, classes, horizon), f32),
            V((two, 8, horizon), f32),
            V((two, nr, 8, horizon), f32),
            V((two, 8, horizon), f32),
            V((two, np_, 8, horizon), f32),
            dma((nr,)), dma((nr,)), dma((nr,)), dma((nr,)),
            dma((np_,)), dma((np_,)), dma((np_,)), dma((np_,)),
            dma((two, np_)), dma((two, np_)), dma((two, np_)), dma((two, np_)),
            dma((two, nr)), dma((two, nr)), dma((two, np_)), dma((two, np_)),
            dma((two, nr)), dma((two, nr)), dma((two, np_)), dma((two, np_)),
        ],
        compiler_params=pltpu.CompilerParams(
            collective_id=0, has_side_effects=True, vmem_limit_bytes=60 * 1024 * 1024),
    )(par, kidx, mask, bottom, dt, u, z, v, wt, at, rs, p2, pt2, e2)


def solution(mesh):
    return jax.shard_map(
        functools.partial(on_device, mesh.shape["reg"], mesh.shape["prod"]),
        mesh=mesh,
        in_specs=(
            P("reg", "prod", None),
            P("reg", "prod", None),
            P("reg", "prod", None),
            P("reg", None, None),
            P("reg", "prod"),
            P("reg", "prod"),
            P("reg", "prod"),
            P("reg", None),
            P(),
            P(),
        ),
        out_specs=(P("reg", "prod", None), P("reg", "prod", None)),
        check_vma=False,
    )
```

```python
import functools

import jax
import jax.numpy as jnp
from jax import lax
from jax.experimental import pallas as pl
from jax.experimental.pallas import tpu as pltpu
from jax.sharding import PartitionSpec as P

MESH = pl.DeviceIdType.MESH
ITERATIONS = 2
LANES = 128


def steps(lo, hi, f, c, block=8):
    count = hi - lo
    if count <= block:
        for i in range(lo, hi):
            c = f(i, c)
        return c
    if count % block:
        return lax.fori_loop(lo, hi, f, c)

    def several(i, c):
        for j in range(block):
            c = f(lo + i * block + j, c)
        return c

    return lax.fori_loop(0, count // block, several, c)


def halves(x):
    hi = x.astype(jnp.bfloat16)
    lo = (x - hi.astype(jnp.float32)).astype(jnp.bfloat16)
    return jnp.concatenate([hi, lo], axis=0)


def apply_map(map2, x):
    return jnp.dot(map2, halves(x), preferred_element_type=jnp.float32)


def kernel(
    nr, np_, shared, per_tile,
    par_ref, kidx_ref, mask_ref,
    b_ref, dt_ref, u_ref, z_ref, v_ref, wt_ref, at_ref, rs_ref, p2_ref, pt2_ref, e2_ref,
    x_ref, res_ref,
    wt_buf, at_buf, uz_buf, g0_buf, uz_send,
    db, wcol, wgi, wgc, r0_buf, img0, img1,
    col_send, rs_buf, own, vbuf, gbuf, row_send, row_buf, rows_w, cor_send, cor_half, cor_buf, zed,
    sc_send, sc_buf, sd_send, sd_buf,
    s_w, r_w, s_uz, r_uz, s_a, r_a, s_v, r_v,
    s_rs, r_rs, s_ag, r_ag, s_row, r_row, s_cor, r_cor, s_sc, r_sc, s_sd, r_sd,
):
    regions, items, horizon = b_ref.shape
    classes = p2_ref.shape[0]
    slab = regions // np_
    gs = u_ref.shape[0]
    mr = lax.axis_index("reg")
    mp = lax.axis_index("prod")

    def to(axis, me, n, s):
        return {axis: lax.rem(me + s, n)}

    def reg_copy(src, dst, ss, rr, s):
        return pltpu.make_async_remote_copy(
            src_ref=src, dst_ref=dst, send_sem=ss, recv_sem=rr,
            device_id=to("reg", mr, nr, s), device_id_type=MESH)

    def prod_copy(src, dst, ss, rr, s):
        return pltpu.make_async_remote_copy(
            src_ref=src, dst_ref=dst, send_sem=ss, recv_sem=rr,
            device_id=to("prod", mp, np_, s), device_id_type=MESH)

    half = np_ // 2
    local = lax.rem(mp, half)
    home = mp - local
    other = lax.rem(mp + half, np_)

    def mate(s):
        return home + lax.rem(local + s, half)

    def giver(s):
        return home + lax.rem(local + half - s, half)

    def across(i):
        return lax.rem(i + half, np_)

    def each_mate(f):
        steps(1, half, lambda s, c: (f(s), c)[1], 0)

    def copy_to(i, src, dst, ss, rr):
        return pltpu.make_async_remote_copy(
            src_ref=src, dst_ref=dst, send_sem=ss, recv_sem=rr,
            device_id={"prod": i}, device_id_type=MESH)

    barrier = pltpu.get_barrier_semaphore()
    for s in range(1, nr):
        pl.semaphore_signal(barrier, inc=1, device_id=to("reg", mr, nr, s), device_id_type=MESH)

    def greet(s, c):
        pl.semaphore_signal(barrier, inc=1, device_id=to("prod", mp, np_, s), device_id_type=MESH)
        return c

    steps(1, np_, greet, 0)
    for g in range(gs):
        uz_send[g] = u_ref[g] + apply_map(pt2_ref[...], z_ref[g])
    pl.semaphore_wait(barrier, nr - 1 + np_ - 1)

    def each_prod(f):
        steps(1, np_, lambda s, c: (f(s), c)[1], 0)

    def w_copy(s):
        return reg_copy(wt_ref, wt_buf.at[s], s_w.at[s], r_w.at[s], s)

    def uz_copy(s):
        return reg_copy(uz_send, uz_buf.at[pl.ds(mr * gs, gs)], s_uz.at[s], r_uz.at[s], s)

    def a_copy(s):
        return prod_copy(at_ref, at_buf.at[mp], s_a.at[s], r_a.at[s], s)

    def v_cross():
        return copy_to(other, v_ref, g0_buf.at[mp], s_v.at[0], r_v.at[0])

    def v_copy(s):
        return copy_to(mate(s), v_ref, g0_buf.at[mp], s_v.at[s], r_v.at[s])

    def v_pass(s):
        return copy_to(mate(s), g0_buf.at[other], g0_buf.at[other], s_v.at[half + s], r_v.at[half + s])

    for s in range(1, nr):
        w_copy(s).start()
    v_cross().start()
    each_mate(lambda s: v_copy(s).start())
    for s in range(1, nr):
        uz_copy(s).start()
    each_prod(lambda s: a_copy(s).start())
    g0_buf[mp] = v_ref[...]
    at_buf[mp] = at_ref[...]
    for g in range(gs):
        uz_buf[mr * gs + g] = uz_send[g]
    base = dt_ref[...]
    v_cross().wait_recv()
    each_mate(lambda s: v_pass(s).start())
    for r in range(regions):
        r0_buf[r] = jnp.broadcast_to(base[:, r : r + 1], (items, horizon)) * b_ref[r]
    total = wt_ref[...]
    for s in range(1, nr):
        w_copy(s).wait_recv()
        total = total + wt_buf[s]
    weights = jnp.dot(total, rs_ref[...], precision=lax.Precision.HIGHEST, preferred_element_type=jnp.float32)
    diag = base + weights[:items]
    for r in range(regions):
        db[r] = jnp.broadcast_to(diag[:, r : r + 1], (items, horizon))
    for k in range(shared):
        wgi[k] = jnp.broadcast_to(weights[:items, regions + k : regions + k + 1], (items, horizon))
        wgc[k] = jnp.broadcast_to(weights[items:, regions + k : regions + k + 1], (classes, horizon))

    each_prod(lambda s: a_copy(s).wait_recv())
    tiles = []
    for first in range(0, np_, per_tile):
        tile = at_buf[first]
        for j in range(first + 1, first + per_tile):
            tile = tile + at_buf[j]
        tiles.append(tile)
    wac = jnp.concatenate(tiles, axis=0) + weights[items:]
    lane = lax.broadcasted_iota(jnp.int32, (classes, LANES), 1)
    for i in range(slab):
        column = jnp.sum(jnp.where(lane == mp * slab + i, wac, 0.0), axis=1, keepdims=True)
        wcol[i] = jnp.broadcast_to(column, (classes, horizon))

    for s in range(1, nr):
        uz_copy(s).wait_recv()
    each_mate(lambda s: v_copy(s).wait_recv())
    each_mate(lambda s: v_pass(s).wait_recv())

    def first_field(a, c):
        flat = jnp.concatenate([g0_buf[j, a] for j in range(np_)], axis=0)
        lifted = apply_map(e2_ref[...], flat)
        for t in range(per_tile):
            r = a * per_tile + t
            r0_buf[r] = r0_buf[r] + uz_buf[par_ref[r]] + lifted[t * items : (t + 1) * items]
        return c

    steps(0, regions // per_tile, first_field, 0)

    row_id = lax.broadcasted_iota(jnp.int32, (8, horizon), 0)
    norm_was = alpha_was = None
    for op in range(ITERATIONS):
        field = r0_buf if op == 0 else res_ref
        image = img0 if op == 0 else img1

        def row_copy(s, op=op):
            return reg_copy(row_send.at[op], row_buf.at[op, s], s_row.at[op, s], r_row.at[op, s], s)

        def rs_copy(s, slot, op=op):
            return copy_to(mate(s), col_send.at[op, slot], rs_buf.at[op, slot], s_rs.at[op, slot], r_rs.at[op, slot])

        def rs_cross(op=op):
            return copy_to(other, col_send.at[op, 0], rs_buf.at[op, 0], s_rs.at[op, 0], r_rs.at[op, 0])

        def cor_copy(s, op=op):
            return copy_to(mate(s), cor_send.at[op], cor_buf.at[op, s], s_cor.at[op, s], r_cor.at[op, s])

        def cor_cross(op=op):
            return copy_to(other, cor_half.at[op], cor_buf.at[op, 0], s_cor.at[op, 0], r_cor.at[op, 0])

        def mine(i):
            return pl.ds(i * slab, slab)

        def ag_copy(s, op=op):
            return copy_to(mate(s), vbuf.at[op], gbuf.at[op, mine(mp)], s_ag.at[op, s], r_ag.at[op, s])

        def ag_cross(op=op):
            return copy_to(other, vbuf.at[op], gbuf.at[op, mine(mp)], s_ag.at[op, 0], r_ag.at[op, 0])

        def ag_pass(s, op=op):
            block = gbuf.at[op, mine(other)]
            return copy_to(mate(s), block, block, s_ag.at[op, half + s], r_ag.at[op, half + s])

        def sc_copy(s, op=op):
            return reg_copy(sc_send.at[op], sc_buf.at[op, s], s_sc.at[op, s], r_sc.at[op, s], s)

        def sd_copy(s, op=op):
            return prod_copy(sd_send.at[op], sd_buf.at[op, s], s_sd.at[op, s], r_sd.at[op, s], s)

        def one_row(k, c, op=op, field=field):
            def add(r, acc):
                return acc + jnp.where(kidx_ref[r] == k, mask_ref[r], 0.0) * field[r]

            row_send[op, k] = steps(0, regions, add, jnp.zeros((items, horizon), jnp.float32), 32)
            return c

        steps(0, shared, one_row, 0)
        for s in range(1, nr):
            row_copy(s).start()

        def columns(i, field=field):
            first = i * slab
            wide = jnp.concatenate([field[first + i] for i in range(slab)], axis=1)
            out = apply_map(p2_ref[...], wide)
            return [out[:, i * horizon : (i + 1) * horizon] for i in range(slab)]

        def send_columns(s, slot, owner, op=op):
            for i, one in enumerate(columns(owner)):
                col_send[op, slot, i] = one
            rs_copy(s, slot).start()

        each_mate(lambda s: send_columns(s, half + s, across(mate(s))))
        each_mate(lambda s: send_columns(s, s, mate(s)))
        for i, one in enumerate(columns(mp)):
            own[i] = one
        theirs = columns(other)

        for s in range(1, nr):
            row_copy(s).wait_recv()

        def one_corner(k, acc, op=op):
            rows = row_send[op, k]
            for s in range(1, nr):
                rows = rows + row_buf[op, s, k]
            weighted = wgi[k] * rows
            rows_w[k] = weighted
            cor_send[op, k] = apply_map(p2_ref[...], rows)
            return acc + weighted * rows

        row_part = steps(0, shared, one_corner, jnp.zeros((items, horizon), jnp.float32))
        each_mate(lambda s: cor_copy(s).start())

        each_mate(lambda s: rs_copy(s, half + s).wait_recv())
        for i in range(slab):
            col_send[op, 0, i] = steps(1, half, lambda s, c, i=i, op=op: c + rs_buf[op, half + s, i], theirs[i])
        rs_cross().start()

        each_mate(lambda s: cor_copy(s).wait_recv())

        def half_corner(k, c, op=op):
            cor_half[op, k] = steps(1, half, lambda s, t: t + cor_buf[op, s, k], cor_send[op, k])
            return c

        steps(0, shared, half_corner, 0)
        cor_cross().start()

        def diagonal(r, acc, field=field, image=image):
            v = field[r]
            w = db[r] * v
            image[r] = w
            return acc[0] + v * v, acc[1] + w * v

        zero = jnp.zeros((items, horizon), jnp.float32)
        norm_part, along_part = steps(0, regions, diagonal, (zero, zero))
        along_part = along_part + row_part * (1.0 / nr)

        cor_cross().wait_recv()

        def one_zed(k, acc, op=op):
            corner = cor_half[op, k] + cor_buf[op, 0, k]
            weighted = wgc[k] * corner
            zed[k] = weighted
            return acc + weighted * corner

        czero = jnp.zeros((classes, horizon), jnp.float32)
        cor_part = steps(0, shared, one_zed, czero) * (1.0 / (nr * np_))

        each_mate(lambda s: rs_copy(s, s).wait_recv())
        rs_cross().wait_recv()
        for i in range(slab):
            r = mp * slab + i
            cols = steps(0, half, lambda s, c, i=i, op=op: c + rs_buf[op, s, i], own[i])
            weighted = wcol[i] * cols
            cor_part = cor_part + weighted * cols
            value = weighted + mask_ref[r] * zed[kidx_ref[r]]
            vbuf[op, i] = value
            gbuf[op, r] = value
        ag_cross().start()
        each_mate(lambda s: ag_copy(s).start())

        def fold(x):
            return jnp.sum(x, axis=0, keepdims=True)

        along_row = fold(along_part) + fold(cor_part)
        sc_send[op] = jnp.where(row_id == 0, fold(norm_part), jnp.where(row_id == 1, along_row, 0.0))
        for s in range(1, nr):
            sc_copy(s).start()
        ag_cross().wait_recv()
        each_mate(lambda s: ag_pass(s).start())
        tally = sc_send[op]
        for s in range(1, nr):
            sc_copy(s).wait_recv()
            tally = tally + sc_buf[op, s]
        sd_send[op] = tally
        each_prod(lambda s: sd_copy(s).start())

        def lift(first, op=op, image=image):
            wide = jnp.concatenate([gbuf[op, first + i] for i in range(slab)], axis=1)
            out = apply_map(pt2_ref[...], wide)
            for i in range(slab):
                r = first + i
                image[r] = (image[r] + mask_ref[r] * rows_w[kidx_ref[r]]) + out[:, i * horizon : (i + 1) * horizon]

        lift(mp * slab)
        lift(other * slab)

        def take(s):
            ag_copy(s).wait_recv()
            lift(giver(s) * slab)

        def take_passed(s):
            ag_pass(s).wait_recv()
            lift(across(giver(s)) * slab)

        each_mate(take)
        each_mate(take_passed)
        each_prod(lambda s: sd_copy(s).wait_recv())
        tally = steps(1, np_, lambda s, c, op=op: c + sd_buf[op, s], sd_send[op])
        norm = jnp.sum(tally[0:1], axis=1, keepdims=True)
        along = jnp.sum(tally[1:2], axis=1, keepdims=True)
        if op == 0:
            alpha = norm / along

            def update(r, c, alpha=alpha):
                res_ref[r] = r0_buf[r] - alpha * img0[r]
                return c

            steps(0, regions, update, 0)
            norm_was, alpha_was = norm, alpha
        else:
            ratio = norm / norm_was
            alpha = norm / (along - ratio * norm / alpha_was)

            def finish(r, c, alpha=alpha, ratio=ratio):
                start, residual = r0_buf[r], res_ref[r]
                x_ref[r] = alpha_was * start + alpha * (residual + ratio * start)
                res_ref[r] = residual - alpha * (img1[r] + ratio * img0[r])
                return c

            steps(0, regions, finish, 0)

        for s in range(1, nr):
            row_copy(s).wait_send()
            sc_copy(s).wait_send()
        each_mate(lambda s: rs_copy(s, s).wait_send())
        each_mate(lambda s: rs_copy(s, half + s).wait_send())
        each_mate(lambda s: cor_copy(s).wait_send())
        each_mate(lambda s: ag_copy(s).wait_send())
        each_mate(lambda s: ag_pass(s).wait_send())
        rs_cross().wait_send()
        cor_cross().wait_send()
        ag_cross().wait_send()
        each_prod(lambda s: sd_copy(s).wait_send())

    for s in range(1, nr):
        w_copy(s).wait_send()
        uz_copy(s).wait_send()
    each_prod(lambda s: a_copy(s).wait_send())
    v_cross().wait_send()
    each_mate(lambda s: v_copy(s).wait_send())
    each_mate(lambda s: v_pass(s).wait_send())


def on_device(nr, np_, bottom, gi_pred, ac_pred, gc_pred, bottom_w, gi_w, ac_w, gc_w, area_table, item_table):
    f32 = jnp.float32
    regions, items, horizon = bottom.shape
    groups, slots = area_table.shape
    classes = item_table.shape[0]
    gs, cs = gi_pred.shape[0], ac_pred.shape[1]
    slab, half = regions // np_, np_ // 2
    per_tile = 8 // cs
    every = regions * nr
    most = min(slots, every - groups + 1)
    shared = 1 + min(groups - 1, every - most - (groups - 1))
    mr, mp = lax.axis_index("reg"), lax.axis_index("prod")

    def member(table, first, count):
        ids = first + jnp.arange(count, dtype=jnp.int32)
        return jnp.any(table[:, :, None] == ids[None, None, :], axis=1)

    area = member(area_table, mr * regions, regions)
    item = member(item_table, mp * items, items)
    sizes = jnp.sum((area_table >= 0).astype(jnp.int32), axis=1)
    ids = jnp.arange(groups, dtype=jnp.int32)
    ahead = (sizes[None, :] > sizes[:, None]) | ((sizes[None, :] == sizes[:, None]) & (ids[None, :] < ids[:, None]))
    rank = jnp.sum(ahead.astype(jnp.int32), axis=1)
    par = jnp.sum(jnp.where(area, ids[:, None], 0), axis=0)
    place = jnp.sum(jnp.where(area, rank[:, None], 0), axis=0)
    mask = (place < shared).astype(f32)
    kidx = jnp.minimum(place, shared - 1)
    single = (area & (rank[:, None] >= shared)).astype(f32)
    chosen = (rank[:, None] == jnp.arange(shared, dtype=jnp.int32)[None, :]).astype(f32)
    rs = jnp.concatenate([single, chosen], axis=1)
    rs = jnp.pad(rs, ((0, LANES - groups), (0, LANES - rs.shape[1])))

    itemf = item.astype(jnp.bfloat16)
    p2 = jnp.concatenate([itemf, itemf], axis=1)
    pt2 = jnp.concatenate([itemf.T, itemf.T], axis=1)
    by_owner = itemf.T.reshape(items, np_, 1, cs)
    eye = jnp.eye(per_tile, dtype=jnp.bfloat16)
    e = (eye[:, None, None, :, None] * by_owner[None]).reshape(per_tile * items, np_ * 8)
    e2 = jnp.concatenate([e, e], axis=1)

    weights = jnp.concatenate([gi_w.T, gc_w.T], axis=0)
    lanes = jnp.arange(LANES, dtype=jnp.int32)
    spread = (lanes[None, :] == mr * gs + jnp.arange(gs, dtype=jnp.int32)[:, None])
    wt = jnp.sum(jnp.where(spread[None], weights[:, :, None], 0.0), axis=1)
    spot = lax.rem(mp, per_tile) * cs + jnp.arange(cs, dtype=jnp.int32)
    rowsel = jnp.arange(8, dtype=jnp.int32)[:, None] == spot[None, :]
    at = jnp.sum(jnp.where(rowsel[:, :, None], ac_w.T[None], 0.0), axis=1)
    at = jnp.pad(at, ((0, 0), (0, LANES - regions)))
    dt = jnp.pad(bottom_w.T, ((0, 0), (0, LANES - regions)))
    u = gi_w[:, :, None] * gi_pred
    z = gc_w[:, :, None] * gc_pred
    v = (ac_w[:, :, None] * ac_pred).reshape(regions // per_tile, 8, horizon)

    field = (regions, items, horizon)
    two = ITERATIONS
    V = pltpu.VMEM
    dma = pltpu.SemaphoreType.DMA
    smem = pl.BlockSpec(memory_space=pltpu.SMEM)
    vmem = pl.BlockSpec(memory_space=pltpu.VMEM)
    return pl.pallas_call(
        functools.partial(kernel, nr, np_, shared, per_tile),
        out_shape=(jax.ShapeDtypeStruct(field, f32), jax.ShapeDtypeStruct(field, f32)),
        in_specs=[smem] * 3 + [vmem] * 11,
        out_specs=(vmem, vmem),
        scratch_shapes=[
            V((nr,) + wt.shape, f32),
            V((np_, 8, LANES), f32),
            V((groups, items, horizon), f32),
            V((np_, regions // per_tile, 8, horizon), f32),
            V((gs, items, horizon), f32),
            V(field, f32),
            V((slab, classes, horizon), f32),
            V((shared, items, horizon), f32),
            V((shared, classes, horizon), f32),
            V(field, f32),
            V(field, f32),
            V(field, f32),
            V((two, np_, slab, classes, horizon), f32),
            V((two, np_, slab, classes, horizon), f32),
            V((slab, classes, horizon), f32),
            V((two, slab, classes, horizon), f32),
            V((two, regions, classes, horizon), f32),
            V((two, shared, items, horizon), f32),
            V((two, nr, shared, items, horizon), f32),
            V((shared, items, horizon), f32),
            V((two, shared, classes, horizon), f32),
            V((two, shared, classes, horizon), f32),
            V((two, half, shared, classes, horizon), f32),
            V((shared, classes, horizon), f32),
            V((two, 8, horizon), f32),
            V((two, nr, 8, horizon), f32),
            V((two, 8, horizon), f32),
            V((two, np_, 8, horizon), f32),
            dma((nr,)), dma((nr,)), dma((nr,)), dma((nr,)),
            dma((np_,)), dma((np_,)), dma((np_,)), dma((np_,)),
            dma((two, np_)), dma((two, np_)), dma((two, np_)), dma((two, np_)),
            dma((two, nr)), dma((two, nr)), dma((two, half)), dma((two, half)),
            dma((two, nr)), dma((two, nr)), dma((two, np_)), dma((two, np_)),
        ],
        compiler_params=pltpu.CompilerParams(
            collective_id=0, has_side_effects=True, vmem_limit_bytes=60 * 1024 * 1024),
    )(par, kidx, mask, bottom, dt, u, z, v, wt, at, rs, p2, pt2, e2)


def solution(mesh):
    return jax.shard_map(
        functools.partial(on_device, mesh.shape["reg"], mesh.shape["prod"]),
        mesh=mesh,
        in_specs=(
            P("reg", "prod", None),
            P("reg", "prod", None),
            P("reg", "prod", None),
            P("reg", None, None),
            P("reg", "prod"),
            P("reg", "prod"),
            P("reg", "prod"),
            P("reg", None),
            P(),
            P(),
        ),
        out_specs=(P("reg", "prod", None), P("reg", "prod", None)),
        check_vma=False,
    )
```

```python
import functools

import jax
import jax.numpy as jnp
from jax import lax
from jax.experimental import pallas as pl
from jax.experimental.pallas import tpu as pltpu
from jax.sharding import PartitionSpec as P

MESH = pl.DeviceIdType.MESH
ITERATIONS = 2
LANES = 128


def steps(lo, hi, f, c, block=8):
    count = hi - lo
    if count <= block:
        for i in range(lo, hi):
            c = f(i, c)
        return c
    if count % block:
        return lax.fori_loop(lo, hi, f, c)

    def several(i, c):
        for j in range(block):
            c = f(lo + i * block + j, c)
        return c

    return lax.fori_loop(0, count // block, several, c)


def halves(x):
    hi = x.astype(jnp.bfloat16)
    lo = (x - hi.astype(jnp.float32)).astype(jnp.bfloat16)
    return jnp.concatenate([hi, lo], axis=0)


def apply_map(map2, x):
    return jnp.dot(map2, halves(x), preferred_element_type=jnp.float32)


def kernel(
    nr, np_, shared, per_tile,
    par_ref, kidx_ref, mask_ref,
    b_ref, dt_ref, u_ref, z_ref, v_ref, wt_ref, at_ref, rs_ref, p2_ref, pt2_ref, e2_ref,
    x_ref, res_ref,
    wt_buf, at_buf, uz_buf, g0_buf, uz_send,
    db, wcol, wgi, wgc, r0_buf, img0, img1,
    col_send, rs_buf, own, vbuf, gbuf, row_send, row_buf, rows_w, cor_send, cor_half, cor_buf, zed,
    sc_send, sc_buf, sd_send, sd_buf,
    s_w, r_w, s_uz, r_uz, s_a, r_a, s_v, r_v,
    s_rs, r_rs, s_ag, r_ag, s_row, r_row, s_cor, r_cor, s_sc, r_sc, s_sd, r_sd,
):
    regions, items, horizon = b_ref.shape
    classes = p2_ref.shape[0]
    slab = regions // np_
    gs = u_ref.shape[0]
    mr = lax.axis_index("reg")
    mp = lax.axis_index("prod")

    def to(axis, me, n, s):
        return {axis: lax.rem(me + s, n)}

    def reg_copy(src, dst, ss, rr, s):
        return pltpu.make_async_remote_copy(
            src_ref=src, dst_ref=dst, send_sem=ss, recv_sem=rr,
            device_id=to("reg", mr, nr, s), device_id_type=MESH)

    def prod_copy(src, dst, ss, rr, s):
        return pltpu.make_async_remote_copy(
            src_ref=src, dst_ref=dst, send_sem=ss, recv_sem=rr,
            device_id=to("prod", mp, np_, s), device_id_type=MESH)

    half = np_ // 2
    local = lax.rem(mp, half)
    home = mp - local
    other = lax.rem(mp + half, np_)

    def mate(s):
        return home + lax.rem(local + s, half)

    def giver(s):
        return home + lax.rem(local + half - s, half)

    def across(i):
        return lax.rem(i + half, np_)

    def each_mate(f):
        steps(1, half, lambda s, c: (f(s), c)[1], 0)

    def copy_to(i, src, dst, ss, rr):
        return pltpu.make_async_remote_copy(
            src_ref=src, dst_ref=dst, send_sem=ss, recv_sem=rr,
            device_id={"prod": i}, device_id_type=MESH)

    barrier = pltpu.get_barrier_semaphore()
    for s in range(1, nr):
        pl.semaphore_signal(barrier, inc=1, device_id=to("reg", mr, nr, s), device_id_type=MESH)

    def greet(s, c):
        pl.semaphore_signal(barrier, inc=1, device_id=to("prod", mp, np_, s), device_id_type=MESH)
        return c

    steps(1, np_, greet, 0)
    for g in range(gs):
        uz_send[g] = u_ref[g] + apply_map(pt2_ref[...], z_ref[g])
    pl.semaphore_wait(barrier, nr - 1 + np_ - 1)

    def each_prod(f):
        steps(1, np_, lambda s, c: (f(s), c)[1], 0)

    def w_copy(s):
        return reg_copy(wt_ref, wt_buf.at[s], s_w.at[s], r_w.at[s], s)

    def uz_copy(s):
        return reg_copy(uz_send, uz_buf.at[pl.ds(mr * gs, gs)], s_uz.at[s], r_uz.at[s], s)

    def a_copy(s):
        return prod_copy(at_ref, at_buf.at[mp], s_a.at[s], r_a.at[s], s)

    def v_cross():
        return copy_to(other, v_ref, g0_buf.at[mp], s_v.at[0], r_v.at[0])

    def v_copy(s):
        return copy_to(mate(s), v_ref, g0_buf.at[mp], s_v.at[s], r_v.at[s])

    def v_pass(s):
        return copy_to(mate(s), g0_buf.at[other], g0_buf.at[other], s_v.at[half + s], r_v.at[half + s])

    for s in range(1, nr):
        w_copy(s).start()
    v_cross().start()
    each_prod(lambda s: a_copy(s).start())
    each_mate(lambda s: v_copy(s).start())
    for s in range(1, nr):
        uz_copy(s).start()
    g0_buf[mp] = v_ref[...]
    at_buf[mp] = at_ref[...]
    for g in range(gs):
        uz_buf[mr * gs + g] = uz_send[g]
    base = dt_ref[...]
    v_cross().wait_recv()
    each_mate(lambda s: v_pass(s).start())
    for r in range(regions):
        r0_buf[r] = jnp.broadcast_to(base[:, r : r + 1], (items, horizon)) * b_ref[r]
    total = wt_ref[...]
    for s in range(1, nr):
        w_copy(s).wait_recv()
        total = total + wt_buf[s]
    weights = jnp.dot(total, rs_ref[...], precision=lax.Precision.HIGHEST, preferred_element_type=jnp.float32)
    diag = base + weights[:items]
    for r in range(regions):
        db[r] = jnp.broadcast_to(diag[:, r : r + 1], (items, horizon))
    for k in range(shared):
        wgi[k] = jnp.broadcast_to(weights[:items, regions + k : regions + k + 1], (items, horizon))
        wgc[k] = jnp.broadcast_to(weights[items:, regions + k : regions + k + 1], (classes, horizon))

    each_prod(lambda s: a_copy(s).wait_recv())
    tiles = []
    for first in range(0, np_, per_tile):
        tile = at_buf[first]
        for j in range(first + 1, first + per_tile):
            tile = tile + at_buf[j]
        tiles.append(tile)
    wac = jnp.concatenate(tiles, axis=0) + weights[items:]
    lane = lax.broadcasted_iota(jnp.int32, (classes, LANES), 1)
    for i in range(slab):
        column = jnp.sum(jnp.where(lane == mp * slab + i, wac, 0.0), axis=1, keepdims=True)
        wcol[i] = jnp.broadcast_to(column, (classes, horizon))

    for s in range(1, nr):
        uz_copy(s).wait_recv()
    each_mate(lambda s: v_copy(s).wait_recv())
    each_mate(lambda s: v_pass(s).wait_recv())

    def first_field(a, c):
        flat = jnp.concatenate([g0_buf[j, a] for j in range(np_)], axis=0)
        lifted = apply_map(e2_ref[...], flat)
        for t in range(per_tile):
            r = a * per_tile + t
            r0_buf[r] = r0_buf[r] + uz_buf[par_ref[r]] + lifted[t * items : (t + 1) * items]
        return c

    steps(0, regions // per_tile, first_field, 0)

    row_id = lax.broadcasted_iota(jnp.int32, (8, horizon), 0)
    norm_was = alpha_was = None
    for op in range(ITERATIONS):
        field = r0_buf if op == 0 else res_ref
        image = img0 if op == 0 else img1

        def row_copy(s, op=op):
            return reg_copy(row_send.at[op], row_buf.at[op, s], s_row.at[op, s], r_row.at[op, s], s)

        def rs_copy(s, slot, op=op):
            return copy_to(mate(s), col_send.at[op, slot], rs_buf.at[op, slot], s_rs.at[op, slot], r_rs.at[op, slot])

        def rs_cross(op=op):
            return copy_to(other, col_send.at[op, 0], rs_buf.at[op, 0], s_rs.at[op, 0], r_rs.at[op, 0])

        def cor_copy(s, op=op):
            return copy_to(mate(s), cor_send.at[op], cor_buf.at[op, s], s_cor.at[op, s], r_cor.at[op, s])

        def cor_cross(op=op):
            return copy_to(other, cor_half.at[op], cor_buf.at[op, 0], s_cor.at[op, 0], r_cor.at[op, 0])

        def mine(i):
            return pl.ds(i * slab, slab)

        def ag_copy(s, op=op):
            return copy_to(mate(s), vbuf.at[op], gbuf.at[op, mine(mp)], s_ag.at[op, s], r_ag.at[op, s])

        def ag_cross(op=op):
            return copy_to(other, vbuf.at[op], gbuf.at[op, mine(mp)], s_ag.at[op, 0], r_ag.at[op, 0])

        def ag_pass(s, op=op):
            block = gbuf.at[op, mine(other)]
            return copy_to(mate(s), block, block, s_ag.at[op, half + s], r_ag.at[op, half + s])

        def sc_copy(s, op=op):
            return reg_copy(sc_send.at[op], sc_buf.at[op, s], s_sc.at[op, s], r_sc.at[op, s], s)

        def sd_copy(s, op=op):
            return prod_copy(sd_send.at[op], sd_buf.at[op, s], s_sd.at[op, s], r_sd.at[op, s], s)

        def one_row(k, c, op=op, field=field):
            def add(r, acc):
                return acc + jnp.where(kidx_ref[r] == k, mask_ref[r], 0.0) * field[r]

            row_send[op, k] = steps(0, regions, add, jnp.zeros((items, horizon), jnp.float32), 32)
            return c

        steps(0, shared, one_row, 0)
        for s in range(1, nr):
            row_copy(s).start()

        def columns(i, field=field):
            first = i * slab
            wide = jnp.concatenate([field[first + i] for i in range(slab)], axis=1)
            out = apply_map(p2_ref[...], wide)
            return [out[:, i * horizon : (i + 1) * horizon] for i in range(slab)]

        def send_columns(s, slot, owner, op=op):
            for i, one in enumerate(columns(owner)):
                col_send[op, slot, i] = one
            rs_copy(s, slot).start()

        each_mate(lambda s: send_columns(s, half + s, across(mate(s))))
        each_mate(lambda s: send_columns(s, s, mate(s)))
        for i, one in enumerate(columns(mp)):
            own[i] = one
        theirs = columns(other)

        for s in range(1, nr):
            row_copy(s).wait_recv()

        def one_corner(k, acc, op=op):
            rows = row_send[op, k]
            for s in range(1, nr):
                rows = rows + row_buf[op, s, k]
            weighted = wgi[k] * rows
            rows_w[k] = weighted
            cor_send[op, k] = apply_map(p2_ref[...], rows)
            return acc + weighted * rows

        row_part = steps(0, shared, one_corner, jnp.zeros((items, horizon), jnp.float32))
        each_mate(lambda s: cor_copy(s).start())

        each_mate(lambda s: rs_copy(s, half + s).wait_recv())
        for i in range(slab):
            col_send[op, 0, i] = steps(1, half, lambda s, c, i=i, op=op: c + rs_buf[op, half + s, i], theirs[i])
        rs_cross().start()

        each_mate(lambda s: cor_copy(s).wait_recv())

        def half_corner(k, c, op=op):
            cor_half[op, k] = steps(1, half, lambda s, t: t + cor_buf[op, s, k], cor_send[op, k])
            return c

        steps(0, shared, half_corner, 0)
        cor_cross().start()

        def diagonal(r, acc, field=field, image=image):
            v = field[r]
            w = db[r] * v
            image[r] = w
            return acc[0] + v * v, acc[1] + w * v

        zero = jnp.zeros((items, horizon), jnp.float32)
        norm_part, along_part = steps(0, regions, diagonal, (zero, zero))
        along_part = along_part + row_part * (1.0 / nr)

        cor_cross().wait_recv()

        def one_zed(k, acc, op=op):
            corner = cor_half[op, k] + cor_buf[op, 0, k]
            weighted = wgc[k] * corner
            zed[k] = weighted
            return acc + weighted * corner

        czero = jnp.zeros((classes, horizon), jnp.float32)
        cor_part = steps(0, shared, one_zed, czero) * (1.0 / (nr * np_))

        each_mate(lambda s: rs_copy(s, s).wait_recv())
        rs_cross().wait_recv()
        for i in range(slab):
            r = mp * slab + i
            cols = steps(0, half, lambda s, c, i=i, op=op: c + rs_buf[op, s, i], own[i])
            weighted = wcol[i] * cols
            cor_part = cor_part + weighted * cols
            value = weighted + mask_ref[r] * zed[kidx_ref[r]]
            vbuf[op, i] = value
            gbuf[op, r] = value
        ag_cross().start()
        each_mate(lambda s: ag_copy(s).start())

        def fold(x):
            return jnp.sum(x, axis=0, keepdims=True)

        along_row = fold(along_part) + fold(cor_part)
        sc_send[op] = jnp.where(row_id == 0, fold(norm_part), jnp.where(row_id == 1, along_row, 0.0))
        for s in range(1, nr):
            sc_copy(s).start()
        tally = sc_send[op]
        for s in range(1, nr):
            sc_copy(s).wait_recv()
            tally = tally + sc_buf[op, s]
        sd_send[op] = tally
        each_prod(lambda s: sd_copy(s).start())
        ag_cross().wait_recv()
        each_mate(lambda s: ag_pass(s).start())

        def lift(first, op=op, image=image):
            wide = jnp.concatenate([gbuf[op, first + i] for i in range(slab)], axis=1)
            out = apply_map(pt2_ref[...], wide)
            for i in range(slab):
                r = first + i
                image[r] = (image[r] + mask_ref[r] * rows_w[kidx_ref[r]]) + out[:, i * horizon : (i + 1) * horizon]

        lift(mp * slab)
        lift(other * slab)

        def take(s):
            ag_copy(s).wait_recv()
            lift(giver(s) * slab)

        def take_passed(s):
            ag_pass(s).wait_recv()
            lift(across(giver(s)) * slab)

        each_mate(take)
        each_mate(take_passed)
        each_prod(lambda s: sd_copy(s).wait_recv())
        tally = steps(1, np_, lambda s, c, op=op: c + sd_buf[op, s], sd_send[op])
        norm = jnp.sum(tally[0:1], axis=1, keepdims=True)
        along = jnp.sum(tally[1:2], axis=1, keepdims=True)
        if op == 0:
            alpha = norm / along

            def update(r, c, alpha=alpha):
                res_ref[r] = r0_buf[r] - alpha * img0[r]
                return c

            steps(0, regions, update, 0)
            norm_was, alpha_was = norm, alpha
        else:
            ratio = norm / norm_was
            alpha = norm / (along - ratio * norm / alpha_was)

            def finish(r, c, alpha=alpha, ratio=ratio):
                start, residual = r0_buf[r], res_ref[r]
                x_ref[r] = alpha_was * start + alpha * (residual + ratio * start)
                res_ref[r] = residual - alpha * (img1[r] + ratio * img0[r])
                return c

            steps(0, regions, finish, 0)

        for s in range(1, nr):
            row_copy(s).wait_send()
            sc_copy(s).wait_send()
        each_mate(lambda s: rs_copy(s, s).wait_send())
        each_mate(lambda s: rs_copy(s, half + s).wait_send())
        each_mate(lambda s: cor_copy(s).wait_send())
        each_mate(lambda s: ag_copy(s).wait_send())
        each_mate(lambda s: ag_pass(s).wait_send())
        rs_cross().wait_send()
        cor_cross().wait_send()
        ag_cross().wait_send()
        each_prod(lambda s: sd_copy(s).wait_send())

    for s in range(1, nr):
        w_copy(s).wait_send()
        uz_copy(s).wait_send()
    each_prod(lambda s: a_copy(s).wait_send())
    v_cross().wait_send()
    each_mate(lambda s: v_copy(s).wait_send())
    each_mate(lambda s: v_pass(s).wait_send())


def on_device(nr, np_, bottom, gi_pred, ac_pred, gc_pred, bottom_w, gi_w, ac_w, gc_w, area_table, item_table):
    f32 = jnp.float32
    regions, items, horizon = bottom.shape
    groups, slots = area_table.shape
    classes = item_table.shape[0]
    gs, cs = gi_pred.shape[0], ac_pred.shape[1]
    slab, half = regions // np_, np_ // 2
    per_tile = 8 // cs
    every = regions * nr
    most = min(slots, every - groups + 1)
    shared = 1 + min(groups - 1, every - most - (groups - 1))
    mr, mp = lax.axis_index("reg"), lax.axis_index("prod")

    def member(table, first, count):
        ids = first + jnp.arange(count, dtype=jnp.int32)
        return jnp.any(table[:, :, None] == ids[None, None, :], axis=1)

    area = member(area_table, mr * regions, regions)
    item = member(item_table, mp * items, items)
    sizes = jnp.sum((area_table >= 0).astype(jnp.int32), axis=1)
    ids = jnp.arange(groups, dtype=jnp.int32)
    ahead = (sizes[None, :] > sizes[:, None]) | ((sizes[None, :] == sizes[:, None]) & (ids[None, :] < ids[:, None]))
    rank = jnp.sum(ahead.astype(jnp.int32), axis=1)
    par = jnp.sum(jnp.where(area, ids[:, None], 0), axis=0)
    place = jnp.sum(jnp.where(area, rank[:, None], 0), axis=0)
    mask = (place < shared).astype(f32)
    kidx = jnp.minimum(place, shared - 1)
    single = (area & (rank[:, None] >= shared)).astype(f32)
    chosen = (rank[:, None] == jnp.arange(shared, dtype=jnp.int32)[None, :]).astype(f32)
    rs = jnp.concatenate([single, chosen], axis=1)
    rs = jnp.pad(rs, ((0, LANES - groups), (0, LANES - rs.shape[1])))

    itemf = item.astype(jnp.bfloat16)
    p2 = jnp.concatenate([itemf, itemf], axis=1)
    pt2 = jnp.concatenate([itemf.T, itemf.T], axis=1)
    by_owner = itemf.T.reshape(items, np_, 1, cs)
    eye = jnp.eye(per_tile, dtype=jnp.bfloat16)
    e = (eye[:, None, None, :, None] * by_owner[None]).reshape(per_tile * items, np_ * 8)
    e2 = jnp.concatenate([e, e], axis=1)

    weights = jnp.concatenate([gi_w.T, gc_w.T], axis=0)
    lanes = jnp.arange(LANES, dtype=jnp.int32)
    spread = (lanes[None, :] == mr * gs + jnp.arange(gs, dtype=jnp.int32)[:, None])
    wt = jnp.sum(jnp.where(spread[None], weights[:, :, None], 0.0), axis=1)
    spot = lax.rem(mp, per_tile) * cs + jnp.arange(cs, dtype=jnp.int32)
    rowsel = jnp.arange(8, dtype=jnp.int32)[:, None] == spot[None, :]
    at = jnp.sum(jnp.where(rowsel[:, :, None], ac_w.T[None], 0.0), axis=1)
    at = jnp.pad(at, ((0, 0), (0, LANES - regions)))
    dt = jnp.pad(bottom_w.T, ((0, 0), (0, LANES - regions)))
    u = gi_w[:, :, None] * gi_pred
    z = gc_w[:, :, None] * gc_pred
    v = (ac_w[:, :, None] * ac_pred).reshape(regions // per_tile, 8, horizon)

    field = (regions, items, horizon)
    two = ITERATIONS
    V = pltpu.VMEM
    dma = pltpu.SemaphoreType.DMA
    smem = pl.BlockSpec(memory_space=pltpu.SMEM)
    vmem = pl.BlockSpec(memory_space=pltpu.VMEM)
    return pl.pallas_call(
        functools.partial(kernel, nr, np_, shared, per_tile),
        out_shape=(jax.ShapeDtypeStruct(field, f32), jax.ShapeDtypeStruct(field, f32)),
        in_specs=[smem] * 3 + [vmem] * 11,
        out_specs=(vmem, vmem),
        scratch_shapes=[
            V((nr,) + wt.shape, f32),
            V((np_, 8, LANES), f32),
            V((groups, items, horizon), f32),
            V((np_, regions // per_tile, 8, horizon), f32),
            V((gs, items, horizon), f32),
            V(field, f32),
            V((slab, classes, horizon), f32),
            V((shared, items, horizon), f32),
            V((shared, classes, horizon), f32),
            V(field, f32),
            V(field, f32),
            V(field, f32),
            V((two, np_, slab, classes, horizon), f32),
            V((two, np_, slab, classes, horizon), f32),
            V((slab, classes, horizon), f32),
            V((two, slab, classes, horizon), f32),
            V((two, regions, classes, horizon), f32),
            V((two, shared, items, horizon), f32),
            V((two, nr, shared, items, horizon), f32),
            V((shared, items, horizon), f32),
            V((two, shared, classes, horizon), f32),
            V((two, shared, classes, horizon), f32),
            V((two, half, shared, classes, horizon), f32),
            V((shared, classes, horizon), f32),
            V((two, 8, horizon), f32),
            V((two, nr, 8, horizon), f32),
            V((two, 8, horizon), f32),
            V((two, np_, 8, horizon), f32),
            dma((nr,)), dma((nr,)), dma((nr,)), dma((nr,)),
            dma((np_,)), dma((np_,)), dma((np_,)), dma((np_,)),
            dma((two, np_)), dma((two, np_)), dma((two, np_)), dma((two, np_)),
            dma((two, nr)), dma((two, nr)), dma((two, half)), dma((two, half)),
            dma((two, nr)), dma((two, nr)), dma((two, np_)), dma((two, np_)),
        ],
        compiler_params=pltpu.CompilerParams(
            collective_id=0, has_side_effects=True, vmem_limit_bytes=60 * 1024 * 1024),
    )(par, kidx, mask, bottom, dt, u, z, v, wt, at, rs, p2, pt2, e2)


def solution(mesh):
    return jax.shard_map(
        functools.partial(on_device, mesh.shape["reg"], mesh.shape["prod"]),
        mesh=mesh,
        in_specs=(
            P("reg", "prod", None),
            P("reg", "prod", None),
            P("reg", "prod", None),
            P("reg", None, None),
            P("reg", "prod"),
            P("reg", "prod"),
            P("reg", "prod"),
            P("reg", None),
            P(),
            P(),
        ),
        out_specs=(P("reg", "prod", None), P("reg", "prod", None)),
        check_vma=False,
    )
```
